64 devices in a mesh: dp: 4 (over x, y), tp: 16 (over z, core).
Axes of the slice: x: 2, y: 2, z: 8, core: 2. Of those that a mesh axis runs over, the one named last changes fastest.
The devices are a block of a 4x4x8 slice.
Arguments:
- x_in: bfloat16 [8192, 2048], P('dp'), parts along dimension 0
- h_mid: bfloat16 [8192, 2048], P('dp'), parts along dimension 0
- mean_x: float32 [8192], P('dp'), parts along dimension 0
- rstd_x: float32 [8192], P('dp'), parts along dimension 0
- mean_h: float32 [8192], P('dp'), parts along dimension 0
- rstd_h: float32 [8192], P('dp'), parts along dimension 0
- gain_x: bfloat16 [2048], replicated
- gain_h: bfloat16 [2048], replicated
- w_qkv: bfloat16 [2048, 6144], P(None, 'tp')
- w_out: bfloat16 [16, 128, 2048], P('tp')
- w_gate: bfloat16 [2048, 8192], P(None, 'tp')
- w_up: bfloat16 [2048, 8192], P(None, 'tp')
- w_down: bfloat16 [8192, 2048], P('tp')
- d_out: bfloat16 [8192, 2048], P('dp'), parts along dimension 0
Outputs:
- output 1: bfloat16 [8192, 2048], P('dp'), parts along dimension 0
- output 2: bfloat16 [8192, 6144], P('dp', 'tp'), parts along dimension 0
- output 3: bfloat16 [64, 128, 2048], P(('dp', 'tp')), parts along dimension 0
- output 4: bfloat16 [8192, 8192], P('dp', 'tp'), parts along dimension 0
- output 5: bfloat16 [8192, 8192], P('dp', 'tp'), parts along dimension 0
- output 6: bfloat16 [32768, 2048], P(('dp', 'tp')), parts along dimension 0
There are 4 independent parts. The reference program is written for one: setup_inputs(seed, part) draws one part's arguments, and reference() takes and returns one part's arrays. A program takes and returns all parts, laid end to end along the dimension named above; an argument that names none is the same for every part.
All inputs are finite; a program needn't handle non-finite values.
Results may differ from the reference program's by a relative error of at most 0.0180282.
Values are sent between devices in bfloat16 or wider.
A program may use at most 768 MiB of HBM per device.

```python
import jax
import jax.numpy as jnp
from jax import lax

D = 2048
HEADS = 16
KV_HEADS = 16
HEAD = 128
FF = 8192
TOKENS = 2048

GROUP_SIZE = HEADS // KV_HEADS
QKV_COLS = (HEADS + 2 * KV_HEADS) * HEAD


def norm_stats(src_rows):
    row_vals = src_rows.astype(jnp.float32)
    row_mean = jnp.mean(row_vals, axis=-1)
    row_var = jnp.mean(jnp.square(row_vals - row_mean[:, None]), axis=-1)
    return row_mean, lax.rsqrt(row_var + 1e-5)


def setup_inputs(seed: int = 0, part: int = 0) -> dict:
    part_keys = jax.random.split(jax.random.fold_in(jax.random.key(seed), part), 7)
    shared_keys = jax.random.split(jax.random.key(seed + 1), 7)
    x_shift = jax.random.normal(part_keys[0], (TOKENS, 1), jnp.float32)
    x_scale = jax.random.uniform(part_keys[1], (TOKENS, 1), jnp.float32, 0.5, 2.0)
    x_in = ((jax.random.normal(part_keys[2], (TOKENS, D), jnp.float32) + x_shift) * x_scale).astype(jnp.bfloat16)
    h_shift = jax.random.normal(part_keys[3], (TOKENS, 1), jnp.float32)
    h_scale = jax.random.uniform(part_keys[4], (TOKENS, 1), jnp.float32, 0.5, 2.0)
    h_mid = ((jax.random.normal(part_keys[5], (TOKENS, D), jnp.float32) + h_shift) * h_scale).astype(jnp.bfloat16)
    d_out = jax.random.normal(part_keys[6], (TOKENS, D), jnp.float32).astype(jnp.bfloat16)
    mean_x, rstd_x = norm_stats(x_in)
    mean_h, rstd_h = norm_stats(h_mid)
    gain_x = (0.6 + 0.8 * jax.random.uniform(shared_keys[0], (D,), jnp.float32)).astype(jnp.bfloat16)
    gain_h = (0.6 + 0.8 * jax.random.uniform(shared_keys[1], (D,), jnp.float32)).astype(jnp.bfloat16)
    w_qkv = (jax.random.normal(shared_keys[2], (D, QKV_COLS), jnp.float32) * D ** -0.5).astype(jnp.bfloat16)
    w_out = (jax.random.normal(shared_keys[3], (HEADS, HEAD, D), jnp.float32) * (HEADS * HEAD) ** -0.5).astype(jnp.bfloat16)
    w_gate = (jax.random.normal(shared_keys[4], (D, FF), jnp.float32) * D ** -0.5).astype(jnp.bfloat16)
    w_up = (jax.random.normal(shared_keys[5], (D, FF), jnp.float32) * D ** -0.5).astype(jnp.bfloat16)
    w_down = (jax.random.normal(shared_keys[6], (FF, D), jnp.float32) * FF ** -0.5).astype(jnp.bfloat16)
    return {'x_in': x_in, 'h_mid': h_mid, 'mean_x': mean_x, 'rstd_x': rstd_x, 'mean_h': mean_h, 'rstd_h': rstd_h, 'gain_x': gain_x, 'gain_h': gain_h, 'w_qkv': w_qkv, 'w_out': w_out, 'w_gate': w_gate, 'w_up': w_up, 'w_down': w_down, 'd_out': d_out}


def layer_norm(src_rows, row_mean, row_rstd, gain_vec):
    centred = (src_rows.astype(jnp.float32) - row_mean[:, None]) * row_rstd[:, None]
    return (centred * gain_vec.astype(jnp.float32)).astype(jnp.bfloat16)


def norm_backward(grad_n, src_rows, row_mean, row_rstd, gain_vec):
    centred = (src_rows.astype(jnp.float32) - row_mean[:, None]) * row_rstd[:, None]
    scaled = grad_n * gain_vec.astype(jnp.float32)
    mean_grad = jnp.mean(scaled, axis=-1, keepdims=True)
    mean_proj = jnp.mean(scaled * centred, axis=-1, keepdims=True)
    return row_rstd[:, None] * (scaled - mean_grad - centred * mean_proj)


def attend(queries, key_rows, value_rows):
    scores = jnp.einsum('tgd,sd->gts', queries, key_rows) * (HEAD ** -0.5)
    positions = jnp.arange(queries.shape[0])
    causal = positions[:, None] >= positions[None, :]
    attn_probs = jax.nn.softmax(jnp.where(causal, scores, -1e30), axis=-1)
    return jnp.einsum('gts,sd->tgd', attn_probs, value_rows)


def group_backward(operands):
    queries, key_rows, value_rows, grad_o = operands
    outputs, pullback = jax.vjp(attend, queries, key_rows, value_rows)
    grad_q, grad_k, grad_v = pullback(grad_o)
    return outputs, grad_q, grad_k, grad_v


def reference(x_in, h_mid, mean_x, rstd_x, mean_h, rstd_h, gain_x, gain_h, w_qkv, w_out, w_gate, w_up, w_down, d_out):
    norm_h = layer_norm(h_mid, mean_h, rstd_h, gain_h)
    gate_f = jnp.dot(norm_h, w_gate, preferred_element_type=jnp.float32).astype(jnp.bfloat16).astype(jnp.float32)
    up_f = jnp.dot(norm_h, w_up, preferred_element_type=jnp.float32).astype(jnp.bfloat16).astype(jnp.float32)
    sig_gate = jax.nn.sigmoid(gate_f)
    gate_act = gate_f * sig_gate
    hidden = (gate_act * up_f).astype(jnp.bfloat16)
    d_w_down = jnp.dot(hidden.T, d_out, preferred_element_type=jnp.float32).astype(jnp.bfloat16)
    d_hidden = jnp.dot(d_out, w_down.T, preferred_element_type=jnp.float32).astype(jnp.bfloat16).astype(jnp.float32)
    d_gate = (d_hidden * up_f * sig_gate * (1.0 + gate_f * (1.0 - sig_gate))).astype(jnp.bfloat16)
    d_up = (d_hidden * gate_act).astype(jnp.bfloat16)
    d_w_gate = jnp.dot(norm_h.T, d_gate, preferred_element_type=jnp.float32).astype(jnp.bfloat16)
    d_w_up = jnp.dot(norm_h.T, d_up, preferred_element_type=jnp.float32).astype(jnp.bfloat16)
    d_norm_h = jnp.dot(d_gate, w_gate.T, preferred_element_type=jnp.float32) + jnp.dot(d_up, w_up.T, preferred_element_type=jnp.float32)
    d_mid = d_out.astype(jnp.float32) + norm_backward(d_norm_h, h_mid, mean_h, rstd_h, gain_h)
    d_mid_b = d_mid.astype(jnp.bfloat16)
    norm_x = layer_norm(x_in, mean_x, rstd_x, gain_x)
    qkv_rows = jnp.dot(norm_x, w_qkv, preferred_element_type=jnp.float32).astype(jnp.bfloat16).astype(jnp.float32)
    qkv_rows = qkv_rows.reshape(TOKENS, KV_HEADS, GROUP_SIZE + 2, HEAD)
    queries = jnp.moveaxis(qkv_rows[:, :, :GROUP_SIZE], 1, 0)
    key_rows = jnp.moveaxis(qkv_rows[:, :, GROUP_SIZE], 1, 0)
    value_rows = jnp.moveaxis(qkv_rows[:, :, GROUP_SIZE + 1], 1, 0)
    d_heads = jnp.dot(d_mid_b, w_out.reshape(HEADS * HEAD, D).T, preferred_element_type=jnp.float32).astype(jnp.bfloat16).astype(jnp.float32)
    grad_o = jnp.moveaxis(d_heads.reshape(TOKENS, KV_HEADS, GROUP_SIZE, HEAD), 1, 0)
    outputs, grad_q, grad_k, grad_v = lax.map(group_backward, (queries, key_rows, value_rows, grad_o))
    attn_out = jnp.moveaxis(outputs, 0, 1).reshape(TOKENS, HEADS * HEAD).astype(jnp.bfloat16)
    d_w_out = jnp.dot(attn_out.T, d_mid_b, preferred_element_type=jnp.float32).astype(jnp.bfloat16).reshape(HEADS, HEAD, D)
    grad_qkv = jnp.concatenate([grad_q, grad_k[:, :, None], grad_v[:, :, None]], axis=2)
    d_qkv = jnp.moveaxis(grad_qkv, 0, 1).reshape(TOKENS, QKV_COLS).astype(jnp.bfloat16)
    d_w_qkv = jnp.dot(norm_x.T, d_qkv, preferred_element_type=jnp.float32).astype(jnp.bfloat16)
    d_norm_x = jnp.dot(d_qkv, w_qkv.T, preferred_element_type=jnp.float32)
    d_x = (d_mid + norm_backward(d_norm_x, x_in, mean_x, rstd_x, gain_x)).astype(jnp.bfloat16)
    return d_x, d_w_qkv, d_w_out, d_w_gate, d_w_up, d_w_down
```

```python
import functools

import jax
import jax.numpy as jnp
from jax import lax
from jax.experimental import pallas as pl
from jax.experimental.pallas import tpu as pltpu
from jax.sharding import PartitionSpec as P

MESH = pl.DeviceIdType.MESH
F32, BF16 = jnp.float32, jnp.bfloat16
NN = (((1,), (0,)), ((), ()))
NT = (((1,), (1,)), ((), ()))
TN = (((0,), (0,)), ((), ()))
SUB = 4
VMEM_BYTES = 67043328


def mm(lhs, rhs, dims=NN):
    return lax.dot_general(lhs, rhs, dims, preferred_element_type=F32)


class Ring:
    def __init__(self, size, tokens):
        me = lax.axis_index("tp")
        self.chips = size // 2
        self.chip, self.core = lax.div(me, 2), lax.rem(me, 2)
        self.way = 1 - 2 * self.core
        self.half, self.rb = tokens // 2, tokens // size
        self.sb = self.rb // SUB
        self.nxt = 2 * lax.rem(self.chip + self.way + self.chips, self.chips) + self.core
        self.prv = 2 * lax.rem(self.chip - self.way + self.chips, self.chips) + self.core
        self.peer = 2 * self.chip + 1 - self.core

    def barrier(self):
        sem = pltpu.get_barrier_semaphore()
        for other in (self.nxt, self.prv, self.peer):
            pl.semaphore_signal(sem, inc=1, device_id={"tp": other}, device_id_type=MESH)
        pl.semaphore_wait(sem, 3)

    def low(self, off):
        return pl.multiple_of(lax.rem(self.chip - off + 2 * self.chips, self.chips) * self.rb, self.rb)

    def high(self, off):
        return pl.multiple_of(self.half + lax.rem(self.chip + off, self.chips) * self.rb, self.rb)

    def mine(self, off, j):
        block = lax.rem(self.chip - self.way * off + 2 * self.chips, self.chips)
        return pl.ds(pl.multiple_of(self.core * self.half + block * self.rb + j * self.sb, self.sb), self.sb)

    def theirs(self, off, j):
        block = lax.rem(self.chip + self.way * off + 2 * self.chips, self.chips)
        return pl.ds(pl.multiple_of((1 - self.core) * self.half + block * self.rb + j * self.sb, self.sb), self.sb)

    def sub(self, j):
        return pl.ds(j * self.sb, self.sb)

    def own_sub(self, j):
        return pl.ds(pl.multiple_of(self.core * self.rb + j * self.sb, self.sb), self.sb)


class Scatter:
    def __init__(self, ring, part, dbuf, pbuf, sbuf, rbuf, dsend, drecv, rsend, rrecv):
        self.ring, self.part, self.dbuf, self.pbuf, self.sbuf, self.rbuf = ring, part, dbuf, pbuf, sbuf, rbuf
        self.dsend, self.drecv, self.rsend, self.rrecv = dsend, drecv, rsend, rrecv

    def pair(self, s):
        return pltpu.make_async_remote_copy(
            src_ref=self.dbuf.at[s], dst_ref=self.pbuf.at[s], send_sem=self.dsend.at[s], recv_sem=self.drecv.at[s],
            device_id={"tp": self.ring.peer}, device_id_type=MESH)

    def hop(self, s, j):
        rows = self.ring.sub(j)
        return pltpu.make_async_remote_copy(
            src_ref=self.sbuf.at[s, rows], dst_ref=self.rbuf.at[s, rows], send_sem=self.rsend.at[s, j], recv_sem=self.rrecv.at[s, j],
            device_id={"tp": self.ring.nxt}, device_id_type=MESH)

    def give(self, s):
        ring = self.ring
        slot = lax.rem(s, 2)
        rows = pl.ds(pl.multiple_of((1 - ring.core) * ring.rb, ring.rb), ring.rb)
        self.dbuf[s] = self.part[slot, rows, :].astype(BF16)
        self.pair(s).start()

    def combine(self, s, j, final):
        ring = self.ring
        slot = lax.rem(s, 2)
        rows = ring.sub(j)
        if j == 0:
            self.pair(s).wait_recv()
        last = ring.chips - 1

        @pl.when(s == 0)
        def _():
            total = self.part[slot, ring.own_sub(j), :] + self.pbuf[s, rows, :].astype(F32)
            self.sbuf[s, rows, :] = total.astype(BF16)
            self.hop(s, j).start()

        @pl.when(jnp.logical_and(s > 0, s < last))
        def _():
            self.hop(s - 1, j).wait_recv()
            total = self.part[slot, ring.own_sub(j), :] + self.pbuf[s, rows, :].astype(F32) + self.rbuf[s - 1, rows, :].astype(F32)
            self.sbuf[s, rows, :] = total.astype(BF16)
            self.hop(s, j).start()

        @pl.when(s == last)
        def _():
            self.hop(s - 1, j).wait_recv()
            total = self.part[slot, ring.own_sub(j), :] + self.pbuf[s, rows, :].astype(F32) + self.rbuf[s - 1, rows, :].astype(F32)
            final(j, total)

    def drain(self):
        def body(s, _):
            self.pair(s).wait_send()

            @pl.when(s < self.ring.chips - 1)
            def _():
                for j in range(SUB):
                    self.hop(s, j).wait_send()
            return 0
        lax.fori_loop(0, self.ring.chips, body, 0)


class Gather:
    def __init__(self, ring, full, asend, arecv, csend, crecv):
        self.ring, self.full = ring, full
        self.asend, self.arecv, self.csend, self.crecv = asend, arecv, csend, crecv

    def hop(self, s, j):
        rows = self.ring.mine(s, j)
        return pltpu.make_async_remote_copy(
            src_ref=self.full.at[rows], dst_ref=self.full.at[rows], send_sem=self.asend.at[s, j], recv_sem=self.arecv.at[s, j],
            device_id={"tp": self.ring.nxt}, device_id_type=MESH)

    def arrival(self, s, j):
        rows = self.ring.mine(s, j)
        return pltpu.make_async_remote_copy(
            src_ref=self.full.at[rows], dst_ref=self.full.at[rows], send_sem=self.asend.at[s - 1, j], recv_sem=self.arecv.at[s - 1, j],
            device_id={"tp": self.ring.nxt}, device_id_type=MESH)

    def across(self, s, j):
        rows = self.ring.mine(s, j)
        return pltpu.make_async_remote_copy(
            src_ref=self.full.at[rows], dst_ref=self.full.at[rows], send_sem=self.csend.at[s, j], recv_sem=self.crecv.at[s, j],
            device_id={"tp": self.ring.peer}, device_id_type=MESH)

    def from_peer(self, s, j):
        rows = self.ring.theirs(s, j)
        return pltpu.make_async_remote_copy(
            src_ref=self.full.at[rows], dst_ref=self.full.at[rows], send_sem=self.csend.at[s, j], recv_sem=self.crecv.at[s, j],
            device_id={"tp": self.ring.peer}, device_id_type=MESH)

    def begin(self, j):
        self.hop(0, j).start()
        self.across(0, j).start()

    def event(self, s, j):
        self.arrival(s, j).wait_recv()

        @pl.when(s < self.ring.chips - 1)
        def _():
            self.hop(s, j).start()
        self.across(s, j).start()

    def settle(self, s):
        for j in range(SUB):
            self.from_peer(s, j).wait_recv()

    def drain(self):
        def body(s, _):
            for j in range(SUB):
                self.across(s, j).wait_send()

            @pl.when(s < self.ring.chips - 1)
            def _():
                for j in range(SUB):
                    self.hop(s, j).wait_send()
            return 0
        lax.fori_loop(0, self.ring.chips, body, 0)


def norm_back(total, src, mean, rstd, gain):
    centred = (src.astype(F32) - mean) * rstd
    scaled = total * gain
    mean_grad = jnp.mean(scaled, axis=-1, keepdims=True)
    mean_proj = jnp.mean(scaled * centred, axis=-1, keepdims=True)
    return rstd * (scaled - mean_grad - centred * mean_proj)


def first_kernel(size, stats, gains, h_hbm, d_hbm, x_hbm, wg_hbm, wu_hbm, wd_hbm, wqkv_hbm, wout_hbm,
                 hid_hbm, dgu_hbm, dqkv_hbm, dwout_hbm, dmid_hbm,
                 wgu, wd, wqkv, wout, hin, din, xin, nrm, gu, dgu, hid, qkv, dqkv, dmid,
                 part, dbuf, pbuf, sbuf, rbuf, full, score, dprob, prob_b, ds_b, k_t, v_t, dk, dv, dwo, dwo_b, q_s, do_s, vec,
                 wsem, insem, outsem, endsem, dsend, drecv, rsend, rrecv, asend, arecv, csend, crecv):
    tokens, depth = h_hbm.shape
    ff = wd_hbm.shape[0]
    head = wout_hbm.shape[0]
    ring = Ring(size, tokens)
    rb, chips = ring.rb, ring.chips
    scatter = Scatter(ring, part, dbuf, pbuf, sbuf, rbuf, dsend, drecv, rsend, rrecv)
    gather = Gather(ring, full, asend, arecv, csend, crecv)
    scale = head ** -0.5

    weights = [pltpu.make_async_copy(wg_hbm, wgu.at[:, pl.ds(0, ff)], wsem.at[0]),
               pltpu.make_async_copy(wu_hbm, wgu.at[:, pl.ds(ff, ff)], wsem.at[1]),
               pltpu.make_async_copy(wd_hbm, wd, wsem.at[2]),
               pltpu.make_async_copy(wqkv_hbm, wqkv, wsem.at[3]),
               pltpu.make_async_copy(wout_hbm, wout, wsem.at[4])]

    def row_loads(t):
        slot = lax.rem(t, 2)
        out = []
        for k, (src, dst) in enumerate(((h_hbm, hin), (d_hbm, din), (x_hbm, xin))):
            for part_no, base in enumerate((ring.low(t + 1), ring.high(t + 1))):
                out.append(pltpu.make_async_copy(src.at[pl.ds(base, rb)], dst.at[slot, pl.ds(part_no * rb, rb)], insem.at[slot, 2 * k + part_no]))
        return out

    def row_stores(t):
        slot = lax.rem(t, 2)
        out = []
        for k, (src, dst) in enumerate(((hid, hid_hbm), (dgu, dgu_hbm))):
            for part_no, base in enumerate((ring.low(t + 1), ring.high(t + 1))):
                out.append(pltpu.make_async_copy(src.at[slot, pl.ds(part_no * rb, rb)], dst.at[pl.ds(base, rb)], outsem.at[slot, 2 * k + part_no]))
        return out

    for copy in row_loads(0):
        copy.start()
    for copy in weights:
        copy.start()
    for copy in row_loads(1):
        copy.start()
    ring.barrier()

    def normed(src, slot, t, col, gain_row):
        for part_no, base in enumerate((ring.low(t + 1), ring.high(t + 1))):
            rows = pl.ds(part_no * rb, rb)
            st = stats[pl.ds(base, rb), :]
            val = (src[slot, rows, :].astype(F32) - st[:, col:col + 1]) * st[:, col + 1:col + 2]
            nrm[rows, :] = (val * gains[gain_row:gain_row + 1, :]).astype(BF16)

    def piece(j, t):
        slot = lax.rem(t, 2)
        if j == 0:
            for copy in row_loads(t):
                copy.wait()
            normed(hin, slot, t, 2, 0)

            @pl.when(t == 0)
            def _():
                weights[0].wait()
                weights[1].wait()
            gu[...] = mm(nrm[...], wgu[...]).astype(BF16)
        elif j == 1:
            @pl.when(t == 0)
            def _():
                weights[2].wait()

            @pl.when(t >= 2)
            def _():
                for copy in row_stores(t - 2):
                    copy.wait()
            d_hidden = mm(din[slot], wd[...], NT).astype(BF16).astype(F32)
            gate_f = gu[:, :ff].astype(F32)
            up_f = gu[:, ff:].astype(F32)
            sig = 1.0 / (1.0 + jnp.exp(-gate_f))
            act = gate_f * sig
            hid[slot] = (act * up_f).astype(BF16)
            dgu[slot, :, :ff] = (d_hidden * up_f * sig * (1.0 + gate_f * (1.0 - sig))).astype(BF16)
            dgu[slot, :, ff:] = (d_hidden * act).astype(BF16)
            for copy in row_stores(t):
                copy.start()
        elif j == 2:
            part[slot] = mm(dgu[slot], wgu[...], NT)
            scatter.give(t)
        else:
            @pl.when(t == 0)
            def _():
                weights[3].wait()
            normed(xin, slot, t, 0, 1)
            val = mm(nrm[...], wqkv[...]).astype(BF16)
            qkv[pl.ds(ring.low(t + 1), rb), :] = val[:rb]
            qkv[pl.ds(ring.high(t + 1), rb), :] = val[rb:]

            @pl.when(t + 2 < chips)
            def _():
                for copy in row_loads(t + 2):
                    copy.start()

    def final(j, total):
        rows = ring.own_sub(j)
        slot = (chips - 1) % 2
        st = stats[ring.mine(0, j), :]
        d_mid = din[slot, rows, :].astype(F32) + norm_back(total, hin[slot, rows, :], st[:, 2:3], st[:, 3:4], gains[0:1, :])
        dmid[ring.sub(j), :] = d_mid
        full[ring.mine(0, j), :] = d_mid.astype(BF16)
        gather.begin(j)

    def rs_body(it, _):
        for j in range(SUB):
            @pl.when(it < chips)
            def _():
                piece(j, it)

            @pl.when(it >= 1)
            def _():
                scatter.combine(it - 1, j, final)
        return 0

    lax.fori_loop(0, chips + 1, rs_body, 0)

    tail = pltpu.make_async_copy(dmid, dmid_hbm, endsem.at[0])
    tail.start()
    k_t[...] = qkv[:, head:2 * head].T
    v_t[...] = qkv[:, 2 * head:3 * head].T
    dk[...] = jnp.zeros_like(dk)
    dv[...] = jnp.zeros_like(dv)
    dwo[...] = jnp.zeros_like(dwo)
    weights[4].wait()

    kc = min(256, tokens)
    hb = xin.at[0]

    def consume(j, s):
        low, high = ring.low(s), ring.high(s)
        if j == 0:
            gather.settle(s)
            hb[pl.ds(0, rb), :] = full[pl.ds(low, rb), :]
            hb[pl.ds(rb, rb), :] = full[pl.ds(high, rb), :]
            q_s[pl.ds(0, rb), :] = qkv[pl.ds(low, rb), 0:head]
            q_s[pl.ds(rb, rb), :] = qkv[pl.ds(high, rb), 0:head]
            do_s[...] = mm(hb[...], wout[...], NT).astype(BF16)
            lane = lax.broadcasted_iota(jnp.int32, (1, 2 * rb), 1)
            pos = jnp.where(lane < rb, low + lane, high - rb + lane)
            peak = jnp.full((1, 2 * rb), -3e38, F32)
            for base in range(0, tokens, kc):
                val = mm(qkv[base:base + kc, head:2 * head], q_s[...], NT)
                key = base + lax.broadcasted_iota(jnp.int32, (kc, 2 * rb), 0)
                val = jnp.where(key <= pos, val, -1e30)
                score[base:base + kc, :] = val
                peak = jnp.maximum(peak, jnp.max(val, axis=0, keepdims=True))
            vec[0:1, :] = peak
        elif j == 1:
            peak = vec[0:1, :]
            norm = jnp.zeros((1, 2 * rb), F32)
            dot = jnp.zeros((1, 2 * rb), F32)
            for base in range(0, tokens, kc):
                val = jnp.exp((score[base:base + kc, :] - peak) * scale)
                d_val = mm(qkv[base:base + kc, 2 * head:3 * head], do_s[...], NT)
                score[base:base + kc, :] = val
                dprob[base:base + kc, :] = d_val
                norm = norm + jnp.sum(val, axis=0, keepdims=True)
                dot = dot + jnp.sum(val * d_val, axis=0, keepdims=True)
            inv = 1.0 / norm
            vec[1:2, :] = inv
            vec[2:3, :] = dot * inv
        elif j == 2:
            inv, row_dot = vec[1:2, :], vec[2:3, :]
            for base in range(0, tokens, kc):
                rows = slice(base, base + kc)
                val = score[rows, :] * inv
                low_p = val.astype(BF16)
                low_d = (val * (dprob[rows, :] - row_dot) * scale).astype(BF16)
                prob_b[rows, :] = low_p
                ds_b[rows, :] = low_d
                dv[rows, :] += mm(low_p, do_s[...])
                dk[rows, :] += mm(low_d, q_s[...])
        else:
            out_t = mm(v_t[...], prob_b[...]).astype(BF16)
            dwo[...] += mm(out_t, hb[...])
            grad_q = mm(k_t[...], ds_b[...]).T.astype(BF16)
            dqkv[pl.ds(low, rb), 0:head] = grad_q[:rb]
            dqkv[pl.ds(high, rb), 0:head] = grad_q[rb:]

    def ag_body(it, _):
        for j in range(SUB):
            consume(j, it - 1)

            @pl.when(it < chips)
            def _():
                gather.event(it, j)
        return 0

    lax.fori_loop(1, chips + 1, ag_body, 0)

    dqkv[:, head:2 * head] = dk[...].astype(BF16)
    dqkv[:, 2 * head:3 * head] = dv[...].astype(BF16)
    dwo_b[...] = dwo[...].astype(BF16)
    ends = [pltpu.make_async_copy(dqkv, dqkv_hbm, endsem.at[1]), pltpu.make_async_copy(dwo_b, dwout_hbm, endsem.at[2])]
    for copy in ends:
        copy.start()
    for copy in row_stores(chips - 2) + row_stores(chips - 1):
        copy.wait()
    tail.wait()
    scatter.drain()
    gather.drain()
    for copy in ends:
        copy.wait()


def second_kernel(size, stats, gains, h_hbm, d_hbm, x_hbm, wqkv_hbm, hid_hbm, dgu_hbm, dqkv_hbm, dmid_hbm,
                  dx_hbm, dwqkv_hbm, dwg_hbm, dwu_hbm, dwd_hbm,
                  wqkv, dqkv, dmid, xown, dgu, hid, hid_t, hcol, dcol, xcol, n_t, ogate, oup, odown, oqkv,
                  part, dbuf, pbuf, sbuf, rbuf, full,
                  wsem, hsem, dsem, xsem, osem, dxsem, dsend, drecv, rsend, rrecv, asend, arecv, csend, crecv):
    tokens, depth = h_hbm.shape
    ff = hid_hbm.shape[1]
    ring = Ring(size, tokens)
    rb, chips = ring.rb, ring.chips
    blk = depth // chips
    scatter = Scatter(ring, part, dbuf, pbuf, sbuf, rbuf, dsend, drecv, rsend, rrecv)
    gather = Gather(ring, full, asend, arecv, csend, crecv)

    own = pl.ds(pl.multiple_of(ring.core * ring.half + ring.chip * rb, rb), rb)
    loads = [pltpu.make_async_copy(dqkv_hbm, dqkv, wsem.at[0]),
             pltpu.make_async_copy(wqkv_hbm, wqkv, wsem.at[1]),
             pltpu.make_async_copy(dgu_hbm, dgu, wsem.at[2]),
             pltpu.make_async_copy(hid_hbm, hid, wsem.at[3]),
             pltpu.make_async_copy(dmid_hbm, dmid, wsem.at[4]),
             pltpu.make_async_copy(x_hbm.at[own], xown, wsem.at[5])]

    def cols(t):
        return pl.ds(pl.multiple_of(t * blk, blk), blk)

    def col_load(src, dst, sem, t):
        slot = lax.rem(t, 2)
        return pltpu.make_async_copy(src.at[:, cols(t)], dst.at[slot], sem.at[slot])

    def store(src, dst, k, t):
        slot = lax.rem(t, 2)
        return pltpu.make_async_copy(src.at[slot], dst.at[cols(t)] if dst is not dwd_hbm else dst.at[:, cols(t)], osem.at[k, slot])

    stores = ((ogate, dwg_hbm, 0), (oup, dwu_hbm, 1), (odown, dwd_hbm, 2), (oqkv, dwqkv_hbm, 3))

    def emit(which, t, value):
        src, dst, k = stores[which]

        @pl.when(t >= 2)
        def _():
            store(src, dst, k, t - 2).wait()
        src[lax.rem(t, 2)] = value.astype(BF16)
        store(src, dst, k, t).start()

    for copy in loads[:4]:
        copy.start()
    col_load(h_hbm, hcol, hsem, 0).start()
    for copy in loads[4:]:
        copy.start()
    ring.barrier()

    def transposed(src, t, col, gain_row):
        val = (src[lax.rem(t, 2)].astype(F32) - stats[:, col:col + 1]) * stats[:, col + 1:col + 2]
        n_t[...] = (val * gains[gain_row:gain_row + 1, cols(t)]).astype(BF16).T

    def piece(j, t):
        slot = lax.rem(t, 2)
        if j == 0:
            @pl.when(t == 0)
            def _():
                loads[0].wait()
                loads[1].wait()
            rows = jnp.concatenate([dqkv[pl.ds(ring.low(t + 1), rb), :], dqkv[pl.ds(ring.high(t + 1), rb), :]], axis=0)
            part[slot] = mm(rows, wqkv[...], NT)
            scatter.give(t)
        elif j == 1:
            @pl.when(t + 1 < chips)
            def _():
                col_load(h_hbm, hcol, hsem, t + 1).start()
            col_load(h_hbm, hcol, hsem, t).wait()
            transposed(hcol, t, 2, 0)
        elif j == 2:
            @pl.when(t == 0)
            def _():
                loads[2].wait()
            emit(0, t, mm(n_t[...], dgu[:, :ff]))
        else:
            emit(1, t, mm(n_t[...], dgu[:, ff:]))

            @pl.when(t == 0)
            def _():
                loads[3].wait()
                hid_t[...] = hid[...].T

            @pl.when(t == chips - 1)
            def _():
                col_load(d_hbm, dcol, dsem, 0).start()
                col_load(x_hbm, xcol, xsem, 0).start()
                loads[4].wait()
                loads[5].wait()

    def final(j, total):
        st = stats[ring.mine(0, j), :]
        rows = ring.sub(j)
        grad = dmid[rows, :] + norm_back(total, xown[rows, :], st[:, 0:1], st[:, 1:2], gains[1:2, :])
        full[ring.mine(0, j), :] = grad.astype(BF16)
        gather.begin(j)

    def rs_body(it, _):
        for j in range(SUB):
            @pl.when(it < chips)
            def _():
                piece(j, it)

            @pl.when(it >= 1)
            def _():
                scatter.combine(it - 1, j, final)
        return 0

    lax.fori_loop(0, chips + 1, rs_body, 0)

    def out_rows(s):
        low, high = ring.low(s), ring.high(s)
        return [pltpu.make_async_copy(full.at[pl.ds(low, rb)], dx_hbm.at[pl.ds(low, rb)], dxsem.at[s, 0]),
                pltpu.make_async_copy(full.at[pl.ds(high, rb)], dx_hbm.at[pl.ds(high, rb)], dxsem.at[s, 1])]

    def consume(j, t):
        if j == 0:
            gather.settle(t)
            for copy in out_rows(t):
                copy.start()

            @pl.when(t + 1 < chips)
            def _():
                col_load(d_hbm, dcol, dsem, t + 1).start()
                col_load(x_hbm, xcol, xsem, t + 1).start()
            col_load(d_hbm, dcol, dsem, t).wait()
            emit(2, t, mm(hid_t[...], dcol[lax.rem(t, 2)]))
        elif j == 1:
            col_load(x_hbm, xcol, xsem, t).wait()
            transposed(xcol, t, 0, 1)
        elif j == 2:
            emit(3, t, mm(n_t[...], dqkv[...]))

    def ag_body(it, _):
        for j in range(SUB):
            consume(j, it - 1)

            @pl.when(it < chips)
            def _():
                gather.event(it, j)
        return 0

    lax.fori_loop(1, chips + 1, ag_body, 0)

    for src, dst, k in stores:
        store(src, dst, k, chips - 2).wait()
        store(src, dst, k, chips - 1).wait()
    scatter.drain()
    gather.drain()

    def finish(s, _):
        for copy in out_rows(s):
            copy.wait()
        return 0
    lax.fori_loop(0, chips, finish, 0)


def solution(mesh):
    size = mesh.shape["tp"]
    chips = size // 2

    def ring_scratch(rb, depth):
        return [pltpu.VMEM((2, 2 * rb, depth), F32), pltpu.VMEM((chips, rb, depth), BF16), pltpu.VMEM((chips, rb, depth), BF16),
                pltpu.VMEM((chips - 1, rb, depth), BF16), pltpu.VMEM((chips - 1, rb, depth), BF16)]

    def ring_sems():
        dma = pltpu.SemaphoreType.DMA
        return [dma((chips,)), dma((chips,)), dma((chips - 1, SUB)), dma((chips - 1, SUB)),
                dma((chips - 1, SUB)), dma((chips - 1, SUB)), dma((chips, SUB)), dma((chips, SUB))]

    def device_step(x_in, h_mid, mean_x, rstd_x, mean_h, rstd_h, gain_x, gain_h, w_qkv, w_out, w_gate, w_up, w_down, d_out):
        tokens, depth = x_in.shape
        head = w_out.shape[1]
        ff = w_gate.shape[1]
        width = w_qkv.shape[1]
        rb = tokens // size
        blk = depth // chips
        dma = pltpu.SemaphoreType.DMA
        stats = jnp.stack([mean_x, rstd_x, mean_h, rstd_h], axis=1)
        gains = jnp.stack([gain_h, gain_x], axis=0).astype(F32)
        any_spec = pl.BlockSpec(memory_space=pl.ANY)
        vmem_spec = pl.BlockSpec(memory_space=pltpu.VMEM)
        shape = jax.ShapeDtypeStruct

        hidden, d_gu, d_qkv, d_w_out, d_mid = pl.pallas_call(
            functools.partial(first_kernel, size),
            out_shape=(shape((tokens, ff), BF16), shape((tokens, 2 * ff), BF16), shape((tokens, width), BF16),
                       shape((head, depth), BF16), shape((rb, depth), F32)),
            in_specs=[vmem_spec] * 2 + [any_spec] * 8,
            out_specs=[any_spec] * 5,
            scratch_shapes=[
                pltpu.VMEM((depth, 2 * ff), BF16), pltpu.VMEM((ff, depth), BF16), pltpu.VMEM((depth, width), BF16), pltpu.VMEM((head, depth), BF16),
                pltpu.VMEM((2, 2 * rb, depth), BF16), pltpu.VMEM((2, 2 * rb, depth), BF16), pltpu.VMEM((2, 2 * rb, depth), BF16),
                pltpu.VMEM((2 * rb, depth), BF16), pltpu.VMEM((2 * rb, 2 * ff), BF16), pltpu.VMEM((2, 2 * rb, 2 * ff), BF16), pltpu.VMEM((2, 2 * rb, ff), BF16),
                pltpu.VMEM((tokens, width), BF16), pltpu.VMEM((tokens, width), BF16), pltpu.VMEM((rb, depth), F32),
                *ring_scratch(rb, depth), pltpu.VMEM((tokens, depth), BF16),
                pltpu.VMEM((tokens, 2 * rb), F32), pltpu.VMEM((tokens, 2 * rb), F32), pltpu.VMEM((tokens, 2 * rb), BF16), pltpu.VMEM((tokens, 2 * rb), BF16),
                pltpu.VMEM((head, tokens), BF16), pltpu.VMEM((head, tokens), BF16), pltpu.VMEM((tokens, head), F32), pltpu.VMEM((tokens, head), F32),
                pltpu.VMEM((head, depth), F32), pltpu.VMEM((head, depth), BF16), pltpu.VMEM((2 * rb, head), BF16), pltpu.VMEM((2 * rb, head), BF16), pltpu.VMEM((8, 2 * rb), F32),
                dma((5,)), dma((2, 6)), dma((2, 4)), dma((3,)), *ring_sems(),
            ],
            compiler_params=pltpu.CompilerParams(collective_id=0, has_side_effects=True, vmem_limit_bytes=VMEM_BYTES),
        )(stats, gains, h_mid, d_out, x_in, w_gate, w_up, w_down, w_qkv, w_out.reshape(head, depth))

        d_x, d_w_qkv, d_w_gate, d_w_up, d_w_down = pl.pallas_call(
            functools.partial(second_kernel, size),
            out_shape=(shape((tokens, depth), BF16), shape((depth, width), BF16), shape((depth, ff), BF16), shape((depth, ff), BF16), shape((ff, depth), BF16)),
            in_specs=[vmem_spec] * 2 + [any_spec] * 8,
            out_specs=[any_spec] * 5,
            scratch_shapes=[
                pltpu.VMEM((depth, width), BF16), pltpu.VMEM((tokens, width), BF16), pltpu.VMEM((rb, depth), F32), pltpu.VMEM((rb, depth), BF16),
                pltpu.VMEM((tokens, 2 * ff), BF16), pltpu.VMEM((tokens, ff), BF16), pltpu.VMEM((ff, tokens), BF16),
                pltpu.VMEM((2, tokens, blk), BF16), pltpu.VMEM((2, tokens, blk), BF16), pltpu.VMEM((2, tokens, blk), BF16), pltpu.VMEM((blk, tokens), BF16),
                pltpu.VMEM((2, blk, ff), BF16), pltpu.VMEM((2, blk, ff), BF16), pltpu.VMEM((2, ff, blk), BF16), pltpu.VMEM((2, blk, width), BF16),
                *ring_scratch(rb, depth), pltpu.VMEM((tokens, depth), BF16),
                dma((6,)), dma((2,)), dma((2,)), dma((2,)), dma((4, 2)), dma((chips, 2)), *ring_sems(),
            ],
            compiler_params=pltpu.CompilerParams(collective_id=1, has_side_effects=True, vmem_limit_bytes=VMEM_BYTES),
        )(stats, gains, h_mid, d_out, x_in, w_qkv, hidden, d_gu, d_qkv, d_mid)
        return d_x, d_w_qkv, d_w_out.reshape(w_out.shape), d_w_gate, d_w_up, d_w_down

    row_spec = P('dp', None)
    stat_spec = P('dp')
    col_spec = P(None, 'tp')
    in_specs = (row_spec, row_spec, stat_spec, stat_spec, stat_spec, stat_spec, P(None), P(None), col_spec, P('tp', None, None), col_spec, col_spec, P('tp', None), row_spec)
    out_specs = (row_spec, P('dp', 'tp'), P(('dp', 'tp'), None, None), P('dp', 'tp'), P('dp', 'tp'), P(('dp', 'tp'), None))
    return jax.shard_map(device_step, mesh=mesh, in_specs=in_specs, out_specs=out_specs, check_vma=False)
```

```python
import functools

import jax
import jax.numpy as jnp
from jax import lax
from jax.experimental import pallas as pl
from jax.experimental.pallas import tpu as pltpu
from jax.sharding import PartitionSpec as P

MESH = pl.DeviceIdType.MESH
F32, BF16 = jnp.float32, jnp.bfloat16
NN = (((1,), (0,)), ((), ()))
NT = (((1,), (1,)), ((), ()))
TN = (((0,), (0,)), ((), ()))
SUB = 4
VMEM_BYTES = 67043328
SECOND_BYTES = 47 * 2 ** 20
COPY_BYTES = 2 * 2 ** 20


def mm(lhs, rhs, dims=NN):
    return lax.dot_general(lhs, rhs, dims, preferred_element_type=F32)


class Ring:
    def __init__(self, size, tokens):
        me = lax.axis_index("tp")
        self.chips = size // 2
        self.chip, self.core = lax.div(me, 2), lax.rem(me, 2)
        self.way = 1 - 2 * self.core
        self.half, self.rb = tokens // 2, tokens // size
        self.sb = self.rb // SUB
        self.nxt = 2 * lax.rem(self.chip + self.way + self.chips, self.chips) + self.core
        self.prv = 2 * lax.rem(self.chip - self.way + self.chips, self.chips) + self.core
        self.peer = 2 * self.chip + 1 - self.core

    def barrier(self):
        sem = pltpu.get_barrier_semaphore()
        for other in (self.nxt, self.prv, self.peer):
            pl.semaphore_signal(sem, inc=1, device_id={"tp": other}, device_id_type=MESH)
        pl.semaphore_wait(sem, 3)

    def low(self, off):
        return pl.multiple_of(lax.rem(self.chip - off + 2 * self.chips, self.chips) * self.rb, self.rb)

    def high(self, off):
        return pl.multiple_of(self.half + lax.rem(self.chip + off, self.chips) * self.rb, self.rb)

    def mine(self, off, j):
        block = lax.rem(self.chip - self.way * off + 2 * self.chips, self.chips)
        return pl.ds(pl.multiple_of(self.core * self.half + block * self.rb + j * self.sb, self.sb), self.sb)

    def theirs(self, off, j):
        block = lax.rem(self.chip + self.way * off + 2 * self.chips, self.chips)
        return pl.ds(pl.multiple_of((1 - self.core) * self.half + block * self.rb + j * self.sb, self.sb), self.sb)

    def sub(self, j):
        return pl.ds(j * self.sb, self.sb)

    def own_sub(self, j):
        return pl.ds(pl.multiple_of(self.core * self.rb + j * self.sb, self.sb), self.sb)


class Scatter:
    def __init__(self, ring, part, dbuf, pbuf, sbuf, rbuf, dsend, drecv, rsend, rrecv):
        self.ring, self.part, self.dbuf, self.pbuf, self.sbuf, self.rbuf = ring, part, dbuf, pbuf, sbuf, rbuf
        self.dsend, self.drecv, self.rsend, self.rrecv = dsend, drecv, rsend, rrecv

    def pair(self, s):
        return pltpu.make_async_remote_copy(
            src_ref=self.dbuf.at[s], dst_ref=self.pbuf.at[s], send_sem=self.dsend.at[s], recv_sem=self.drecv.at[s],
            device_id={"tp": self.ring.peer}, device_id_type=MESH)

    def hop(self, s, j):
        rows = self.ring.sub(j)
        return pltpu.make_async_remote_copy(
            src_ref=self.sbuf.at[s, rows], dst_ref=self.rbuf.at[s, rows], send_sem=self.rsend.at[s, j], recv_sem=self.rrecv.at[s, j],
            device_id={"tp": self.ring.nxt}, device_id_type=MESH)

    def give(self, s):
        ring = self.ring
        slot = lax.rem(s, 2)
        rows = pl.ds(pl.multiple_of((1 - ring.core) * ring.rb, ring.rb), ring.rb)
        self.dbuf[s] = self.part[slot, rows, :].astype(BF16)
        self.pair(s).start()

    def combine(self, s, j, final):
        ring = self.ring
        slot = lax.rem(s, 2)
        rows = ring.sub(j)
        if j == 0:
            self.pair(s).wait_recv()
        last = ring.chips - 1

        @pl.when(s == 0)
        def _():
            total = self.part[slot, ring.own_sub(j), :] + self.pbuf[s, rows, :].astype(F32)
            self.sbuf[s, rows, :] = total.astype(BF16)
            self.hop(s, j).start()

        @pl.when(jnp.logical_and(s > 0, s < last))
        def _():
            self.hop(s - 1, j).wait_recv()
            total = self.part[slot, ring.own_sub(j), :] + self.pbuf[s, rows, :].astype(F32) + self.rbuf[s - 1, rows, :].astype(F32)
            self.sbuf[s, rows, :] = total.astype(BF16)
            self.hop(s, j).start()

        @pl.when(s == last)
        def _():
            self.hop(s - 1, j).wait_recv()
            total = self.part[slot, ring.own_sub(j), :] + self.pbuf[s, rows, :].astype(F32) + self.rbuf[s - 1, rows, :].astype(F32)
            final(j, total)

    def drain(self):
        def body(s, _):
            self.pair(s).wait_send()

            @pl.when(s < self.ring.chips - 1)
            def _():
                for j in range(SUB):
                    self.hop(s, j).wait_send()
            return 0
        lax.fori_loop(0, self.ring.chips, body, 0)


class Gather:
    def __init__(self, ring, full, asend, arecv, csend, crecv):
        self.ring, self.full = ring, full
        self.asend, self.arecv, self.csend, self.crecv = asend, arecv, csend, crecv

    def hop(self, s, j):
        rows = self.ring.mine(s, j)
        return pltpu.make_async_remote_copy(
            src_ref=self.full.at[rows], dst_ref=self.full.at[rows], send_sem=self.asend.at[s, j], recv_sem=self.arecv.at[s, j],
            device_id={"tp": self.ring.nxt}, device_id_type=MESH)

    def arrival(self, s, j):
        rows = self.ring.mine(s, j)
        return pltpu.make_async_remote_copy(
            src_ref=self.full.at[rows], dst_ref=self.full.at[rows], send_sem=self.asend.at[s - 1, j], recv_sem=self.arecv.at[s - 1, j],
            device_id={"tp": self.ring.nxt}, device_id_type=MESH)

    def across(self, s, j):
        rows = self.ring.mine(s, j)
        return pltpu.make_async_remote_copy(
            src_ref=self.full.at[rows], dst_ref=self.full.at[rows], send_sem=self.csend.at[s, j], recv_sem=self.crecv.at[s, j],
            device_id={"tp": self.ring.peer}, device_id_type=MESH)

    def from_peer(self, s, j):
        rows = self.ring.theirs(s, j)
        return pltpu.make_async_remote_copy(
            src_ref=self.full.at[rows], dst_ref=self.full.at[rows], send_sem=self.csend.at[s, j], recv_sem=self.crecv.at[s, j],
            device_id={"tp": self.ring.peer}, device_id_type=MESH)

    def begin(self, j):
        self.hop(0, j).start()
        self.across(0, j).start()

    def event(self, s, j):
        self.arrival(s, j).wait_recv()

        @pl.when(s < self.ring.chips - 1)
        def _():
            self.hop(s, j).start()
        self.across(s, j).start()

    def settle(self, s):
        for j in range(SUB):
            self.from_peer(s, j).wait_recv()

    def drain(self):
        def body(s, _):
            for j in range(SUB):
                self.across(s, j).wait_send()

            @pl.when(s < self.ring.chips - 1)
            def _():
                for j in range(SUB):
                    self.hop(s, j).wait_send()
            return 0
        lax.fori_loop(0, self.ring.chips, body, 0)


def stat_columns(sources, dest):
    for k, src in enumerate(sources):
        size, rb = src.shape
        turned = src[...].T
        for b in range(size):
            dest[b * rb:(b + 1) * rb, k:k + 1] = turned[:, b:b + 1]


def gain_rows(sources, dest):
    for k, src in enumerate(sources):
        count, lanes = src.shape
        for b in range(count):
            dest[k:k + 1, b * lanes:(b + 1) * lanes] = src[b:b + 1, :].astype(F32)


def norm_back(total, src, mean, rstd, gain):
    centred = (src.astype(F32) - mean) * rstd
    scaled = total * gain
    mean_grad = jnp.mean(scaled, axis=-1, keepdims=True)
    mean_proj = jnp.mean(scaled * centred, axis=-1, keepdims=True)
    return rstd * (scaled - mean_grad - centred * mean_proj)


def first_kernel(size, mx, rx, mh, rh, gx_in, gh_in, h_hbm, d_hbm, x_hbm, wg_hbm, wu_hbm, wd_hbm, wqkv_hbm, wout_hbm,
                 hid_hbm, dgu_hbm, dqkv_hbm, dwout_hbm, dmid_hbm,
                 stats, gains, wgu, wd, wqkv, wout, hin, din, xin, nrm, gu, dgu, hid, qkv, dqkv, dmid,
                 part, dbuf, pbuf, sbuf, rbuf, full, score, dprob, prob_b, ds_b, k_t, v_t, dk, dv, dwo, dwo_b, q_s, do_s, vec,
                 wsem, insem, outsem, endsem, dsend, drecv, rsend, rrecv, asend, arecv, csend, crecv):
    tokens, depth = h_hbm.shape
    ff = wd_hbm.shape[0]
    head = wout_hbm.shape[0]
    ring = Ring(size, tokens)
    rb, chips = ring.rb, ring.chips
    gx, gh = gains.at[0:1], gains.at[1:2]
    scatter = Scatter(ring, part, dbuf, pbuf, sbuf, rbuf, dsend, drecv, rsend, rrecv)
    gather = Gather(ring, full, asend, arecv, csend, crecv)
    scale = head ** -0.5

    weights = [pltpu.make_async_copy(wg_hbm, wgu.at[:, pl.ds(0, ff)], wsem.at[0]),
               pltpu.make_async_copy(wu_hbm, wgu.at[:, pl.ds(ff, ff)], wsem.at[1]),
               pltpu.make_async_copy(wd_hbm, wd, wsem.at[2]),
               pltpu.make_async_copy(wqkv_hbm, wqkv, wsem.at[3]),
               pltpu.make_async_copy(wout_hbm, wout, wsem.at[4])]

    def row_loads(t):
        slot = lax.rem(t, 2)
        out = []
        for k, (src, dst) in enumerate(((h_hbm, hin), (d_hbm, din), (x_hbm, xin))):
            for part_no, base in enumerate((ring.low(t + 1), ring.high(t + 1))):
                out.append(pltpu.make_async_copy(src.at[pl.ds(base, rb)], dst.at[slot, pl.ds(part_no * rb, rb)], insem.at[slot, 2 * k + part_no]))
        return out

    def row_stores(t):
        slot = lax.rem(t, 2)
        out = []
        for k, (src, dst) in enumerate(((hid, hid_hbm), (dgu, dgu_hbm))):
            for part_no, base in enumerate((ring.low(t + 1), ring.high(t + 1))):
                out.append(pltpu.make_async_copy(src.at[slot, pl.ds(part_no * rb, rb)], dst.at[pl.ds(base, rb)], outsem.at[slot, 2 * k + part_no]))
        return out

    for copy in row_loads(0):
        copy.start()
    for copy in weights:
        copy.start()
    for copy in row_loads(1):
        copy.start()
    ring.barrier()
    stat_columns((mx, rx, mh, rh), stats)
    gain_rows((gx_in, gh_in), gains)

    def normed(src, slot, t, col, gain_ref):
        gain = gain_ref[...]
        for part_no, base in enumerate((ring.low(t + 1), ring.high(t + 1))):
            rows = pl.ds(part_no * rb, rb)
            st = stats[pl.ds(base, rb), :]
            val = (src[slot, rows, :].astype(F32) - st[:, col:col + 1]) * st[:, col + 1:col + 2]
            nrm[rows, :] = (val * gain).astype(BF16)

    def piece(j, t):
        slot = lax.rem(t, 2)
        if j == 0:
            for copy in row_loads(t):
                copy.wait()
            normed(hin, slot, t, 2, gh)

            @pl.when(t == 0)
            def _():
                weights[0].wait()
                weights[1].wait()
            gu[...] = mm(nrm[...], wgu[...]).astype(BF16)
        elif j == 1:
            @pl.when(t == 0)
            def _():
                weights[2].wait()

            @pl.when(t >= 2)
            def _():
                for copy in row_stores(t - 2):
                    copy.wait()
            d_hidden = mm(din[slot], wd[...], NT).astype(BF16).astype(F32)
            gate_f = gu[:, :ff].astype(F32)
            up_f = gu[:, ff:].astype(F32)
            sig = 1.0 / (1.0 + jnp.exp(-gate_f))
            act = gate_f * sig
            hid[slot] = (act * up_f).astype(BF16)
            dgu[slot, :, :ff] = (d_hidden * up_f * sig * (1.0 + gate_f * (1.0 - sig))).astype(BF16)
            dgu[slot, :, ff:] = (d_hidden * act).astype(BF16)
            for copy in row_stores(t):
                copy.start()
        elif j == 2:
            part[slot] = mm(dgu[slot], wgu[...], NT)
            scatter.give(t)
        else:
            @pl.when(t == 0)
            def _():
                weights[3].wait()
            normed(xin, slot, t, 0, gx)
            val = mm(nrm[...], wqkv[...]).astype(BF16)
            qkv[pl.ds(ring.low(t + 1), rb), :] = val[:rb]
            qkv[pl.ds(ring.high(t + 1), rb), :] = val[rb:]

            @pl.when(t + 2 < chips)
            def _():
                for copy in row_loads(t + 2):
                    copy.start()

    def final(j, total):
        rows = ring.own_sub(j)
        slot = (chips - 1) % 2
        st = stats[ring.mine(0, j), :]
        d_mid = din[slot, rows, :].astype(F32) + norm_back(total, hin[slot, rows, :], st[:, 2:3], st[:, 3:4], gh[...])
        dmid[ring.sub(j), :] = d_mid
        full[ring.mine(0, j), :] = d_mid.astype(BF16)
        gather.begin(j)

    def rs_body(it, _):
        for j in range(SUB):
            @pl.when(it >= 1)
            def _():
                scatter.combine(it - 1, j, final)

            @pl.when(it < chips)
            def _():
                piece(j, it)
        return 0

    lax.fori_loop(0, chips + 1, rs_body, 0)

    tail = pltpu.make_async_copy(dmid, dmid_hbm, endsem.at[0])
    tail.start()
    k_t[...] = qkv[:, head:2 * head].T
    v_t[...] = qkv[:, 2 * head:3 * head].T
    dk[...] = jnp.zeros_like(dk)
    dv[...] = jnp.zeros_like(dv)
    dwo[...] = jnp.zeros_like(dwo)
    weights[4].wait()

    kc = min(256, tokens)
    hb = xin.at[0]

    def consume(j, s):
        low, high = ring.low(s), ring.high(s)
        if j == 0:
            gather.settle(s)
            hb[pl.ds(0, rb), :] = full[pl.ds(low, rb), :]
            hb[pl.ds(rb, rb), :] = full[pl.ds(high, rb), :]
            q_s[pl.ds(0, rb), :] = qkv[pl.ds(low, rb), 0:head]
            q_s[pl.ds(rb, rb), :] = qkv[pl.ds(high, rb), 0:head]
            do_s[...] = mm(hb[...], wout[...], NT).astype(BF16)
            lane = lax.broadcasted_iota(jnp.int32, (1, 2 * rb), 1)
            pos = jnp.where(lane < rb, low + lane, high - rb + lane)
            peak = jnp.full((1, 2 * rb), -3e38, F32)
            for base in range(0, tokens, kc):
                val = mm(qkv[base:base + kc, head:2 * head], q_s[...], NT)
                key = base + lax.broadcasted_iota(jnp.int32, (kc, 2 * rb), 0)
                val = jnp.where(key <= pos, val, -1e30)
                score[base:base + kc, :] = val
                peak = jnp.maximum(peak, jnp.max(val, axis=0, keepdims=True))
            vec[0:1, :] = peak
        elif j == 1:
            peak = vec[0:1, :]
            norm = jnp.zeros((1, 2 * rb), F32)
            dot = jnp.zeros((1, 2 * rb), F32)
            for base in range(0, tokens, kc):
                val = jnp.exp((score[base:base + kc, :] - peak) * scale)
                d_val = mm(qkv[base:base + kc, 2 * head:3 * head], do_s[...], NT)
                score[base:base + kc, :] = val
                dprob[base:base + kc, :] = d_val
                norm = norm + jnp.sum(val, axis=0, keepdims=True)
                dot = dot + jnp.sum(val * d_val, axis=0, keepdims=True)
            inv = 1.0 / norm
            vec[1:2, :] = inv
            vec[2:3, :] = dot * inv
        elif j == 2:
            inv, row_dot = vec[1:2, :], vec[2:3, :]
            for base in range(0, tokens, kc):
                rows = slice(base, base + kc)
                val = score[rows, :] * inv
                low_p = val.astype(BF16)
                low_d = (val * (dprob[rows, :] - row_dot) * scale).astype(BF16)
                prob_b[rows, :] = low_p
                ds_b[rows, :] = low_d
                dv[rows, :] += mm(low_p, do_s[...])
                dk[rows, :] += mm(low_d, q_s[...])
        else:
            out_t = mm(v_t[...], prob_b[...]).astype(BF16)
            dwo[...] += mm(out_t, hb[...])
            grad_q = mm(k_t[...], ds_b[...]).T.astype(BF16)
            dqkv[pl.ds(low, rb), 0:head] = grad_q[:rb]
            dqkv[pl.ds(high, rb), 0:head] = grad_q[rb:]

    def ag_body(it, _):
        for j in range(SUB):
            @pl.when(it < chips)
            def _():
                gather.event(it, j)
            consume(j, it - 1)
        return 0

    lax.fori_loop(1, chips + 1, ag_body, 0)

    dqkv[:, head:2 * head] = dk[...].astype(BF16)
    dqkv[:, 2 * head:3 * head] = dv[...].astype(BF16)
    dwo_b[...] = dwo[...].astype(BF16)
    ends = [pltpu.make_async_copy(dqkv, dqkv_hbm, endsem.at[1]), pltpu.make_async_copy(dwo_b, dwout_hbm, endsem.at[2])]
    for copy in ends:
        copy.start()
    for copy in row_stores(chips - 2) + row_stores(chips - 1):
        copy.wait()
    tail.wait()
    scatter.drain()
    gather.drain()
    for copy in ends:
        copy.wait()


def second_kernel(size, mx, rx, mh, rh, gx_in, gh_in, h_hbm, d_hbm, x_hbm, wqkv_hbm, hid_hbm, dgu_hbm, dqkv_hbm, dmid_hbm,
                  full, dwqkv, dwg, dwu, dwd,
                  stats, gains, wqkv, dqkv, dmid, xown, dgu, hid, hid_t, hcol, dcol, xcol, n_t,
                  part, dbuf, pbuf, sbuf, rbuf,
                  wsem, hsem, dsem, xsem, dsend, drecv, rsend, rrecv, asend, arecv, csend, crecv):
    tokens, depth = h_hbm.shape
    ff = hid_hbm.shape[1]
    ring = Ring(size, tokens)
    rb, chips = ring.rb, ring.chips
    gx, gh = gains.at[0:1], gains.at[1:2]
    blk = depth // chips
    scatter = Scatter(ring, part, dbuf, pbuf, sbuf, rbuf, dsend, drecv, rsend, rrecv)
    gather = Gather(ring, full, asend, arecv, csend, crecv)

    own = pl.ds(pl.multiple_of(ring.core * ring.half + ring.chip * rb, rb), rb)
    loads = [pltpu.make_async_copy(dqkv_hbm, dqkv, wsem.at[0]),
             pltpu.make_async_copy(wqkv_hbm, wqkv, wsem.at[1]),
             pltpu.make_async_copy(dgu_hbm, dgu, wsem.at[2]),
             pltpu.make_async_copy(hid_hbm, hid, wsem.at[3]),
             pltpu.make_async_copy(dmid_hbm, dmid, wsem.at[4]),
             pltpu.make_async_copy(x_hbm.at[own], xown, wsem.at[5])]

    def cols(t):
        return pl.ds(pl.multiple_of(t * blk, blk), blk)

    def col_load(src, dst, sem, t):
        slot = lax.rem(t, 2)
        return pltpu.make_async_copy(src.at[:, cols(t)], dst.at[slot], sem.at[slot])

    for copy in loads:
        copy.start()
    col_load(h_hbm, hcol, hsem, 0).start()
    col_load(d_hbm, dcol, dsem, 0).start()
    col_load(x_hbm, xcol, xsem, 0).start()
    ring.barrier()
    stat_columns((mx, rx, mh, rh), stats)
    gain_rows((gx_in, gh_in), gains)

    def transposed(src, t, col, gain_ref):
        val = (src[lax.rem(t, 2)].astype(F32) - stats[:, col:col + 1]) * stats[:, col + 1:col + 2]
        n_t[...] = (val * gain_ref[:, cols(t)]).astype(BF16).T

    def partial(t):
        @pl.when(t == 0)
        def _():
            loads[0].wait()
            loads[1].wait()
        rows = jnp.concatenate([dqkv[pl.ds(ring.low(t + 1), rb), :], dqkv[pl.ds(ring.high(t + 1), rb), :]], axis=0)
        part[lax.rem(t, 2)] = mm(rows, wqkv[...], NT)
        scatter.give(t)

    def fill_mlp(j, t):
        if j == 0:
            @pl.when(t == 0)
            def _():
                for copy in loads[2:]:
                    copy.wait()

            @pl.when(t + 1 < chips)
            def _():
                col_load(h_hbm, hcol, hsem, t + 1).start()
                col_load(d_hbm, dcol, dsem, t + 1).start()
            col_load(h_hbm, hcol, hsem, t).wait()
            transposed(hcol, t, 2, gh)
        elif j == 1:
            dwg[cols(t), :] = mm(n_t[...], dgu[:, :ff]).astype(BF16)
        elif j == 2:
            dwu[cols(t), :] = mm(n_t[...], dgu[:, ff:]).astype(BF16)
        else:
            @pl.when(t == 0)
            def _():
                hid_t[...] = hid[...].T
            col_load(d_hbm, dcol, dsem, t).wait()
            dwd[:, cols(t)] = mm(hid_t[...], dcol[lax.rem(t, 2)]).astype(BF16)

    def fill_qkv(j, t):
        if j == 0:
            @pl.when(t + 1 < chips)
            def _():
                col_load(x_hbm, xcol, xsem, t + 1).start()
            col_load(x_hbm, xcol, xsem, t).wait()
            transposed(xcol, t, 0, gx)
        else:
            dwqkv[cols(t), :] = mm(n_t[...], dqkv[...]).astype(BF16)

    def final(j, total):
        st = stats[ring.mine(0, j), :]
        rows = ring.sub(j)
        grad = dmid[rows, :] + norm_back(total, xown[rows, :], st[:, 0:1], st[:, 1:2], gx[...])
        full[ring.mine(0, j), :] = grad.astype(BF16)
        gather.begin(j)

    partial(0)

    def rs_body(it, _):
        for j in range(SUB):
            scatter.combine(it - 1, j, final)
            if j == 0:
                @pl.when(it < chips)
                def _():
                    partial(it)
            fill_mlp(j, it - 1)
        return 0

    lax.fori_loop(1, chips + 1, rs_body, 0)

    def ag_body(it, _):
        for j in range(SUB):
            gather.event(it, j)
            if j < 2:
                fill_qkv(j, it - 1)
            else:
                @pl.when(it == chips - 1)
                def _():
                    fill_qkv(j - 2, it)
        return 0

    lax.fori_loop(1, chips, ag_body, 0)

    def settle(s, _):
        gather.settle(s)
        return 0
    lax.fori_loop(0, chips, settle, 0)
    scatter.drain()
    gather.drain()


def copy_kernel(dx, dwqkv, dwg, dwu, dwd, dwout_hbm, dx_hbm, dwqkv_hbm, dwg_hbm, dwu_hbm, dwd_hbm, dwout_out, staged, sem):
    first = pltpu.make_async_copy(dwout_hbm, staged, sem.at[0])
    first.start()
    copies = []
    for src, dst in ((dx, dx_hbm), (dwqkv, dwqkv_hbm), (dwg, dwg_hbm), (dwu, dwu_hbm), (dwd, dwd_hbm)):
        copies.append(pltpu.make_async_copy(src, dst, sem.at[len(copies) + 1]))
        copies[-1].start()
    first.wait()
    last = pltpu.make_async_copy(staged, dwout_out, sem.at[6])
    last.start()
    for copy in copies:
        copy.wait()
    last.wait()


def solution(mesh):
    size = mesh.shape["tp"]
    chips = size // 2

    def ring_scratch(rb, depth):
        return [pltpu.VMEM((2, 2 * rb, depth), F32), pltpu.VMEM((chips, rb, depth), BF16), pltpu.VMEM((chips, rb, depth), BF16),
                pltpu.VMEM((chips - 1, rb, depth), BF16), pltpu.VMEM((chips - 1, rb, depth), BF16)]

    def ring_sems():
        dma = pltpu.SemaphoreType.DMA
        return [dma((chips,)), dma((chips,)), dma((chips - 1, SUB)), dma((chips - 1, SUB)),
                dma((chips - 1, SUB)), dma((chips - 1, SUB)), dma((chips, SUB)), dma((chips, SUB))]

    def device_step(x_in, h_mid, mean_x, rstd_x, mean_h, rstd_h, gain_x, gain_h, w_qkv, w_out, w_gate, w_up, w_down, d_out):
        tokens, depth = x_in.shape
        head = w_out.shape[1]
        ff = w_gate.shape[1]
        width = w_qkv.shape[1]
        rb = tokens // size
        blk = depth // chips
        dma = pltpu.SemaphoreType.DMA
        stats = [val.reshape(size, rb) for val in (mean_x, rstd_x, mean_h, rstd_h)]
        gains = [gain_x.reshape(size, depth // size), gain_h.reshape(size, depth // size)]
        any_spec = pl.BlockSpec(memory_space=pl.ANY)
        vmem_spec = pl.BlockSpec(memory_space=pltpu.VMEM)
        shape = jax.ShapeDtypeStruct

        hidden, d_gu, d_qkv, d_w_out, d_mid = pl.pallas_call(
            functools.partial(first_kernel, size),
            out_shape=(shape((tokens, ff), BF16), shape((tokens, 2 * ff), BF16), shape((tokens, width), BF16),
                       shape((head, depth), BF16), shape((rb, depth), F32)),
            in_specs=[vmem_spec] * 6 + [any_spec] * 8,
            out_specs=[any_spec] * 5,
            scratch_shapes=[
                pltpu.VMEM((tokens, 4), F32), pltpu.VMEM((2, depth), F32), pltpu.VMEM((depth, 2 * ff), BF16), pltpu.VMEM((ff, depth), BF16), pltpu.VMEM((depth, width), BF16), pltpu.VMEM((head, depth), BF16),
                pltpu.VMEM((2, 2 * rb, depth), BF16), pltpu.VMEM((2, 2 * rb, depth), BF16), pltpu.VMEM((2, 2 * rb, depth), BF16),
                pltpu.VMEM((2 * rb, depth), BF16), pltpu.VMEM((2 * rb, 2 * ff), BF16), pltpu.VMEM((2, 2 * rb, 2 * ff), BF16), pltpu.VMEM((2, 2 * rb, ff), BF16),
                pltpu.VMEM((tokens, width), BF16), pltpu.VMEM((tokens, width), BF16), pltpu.VMEM((rb, depth), F32),
                *ring_scratch(rb, depth), pltpu.VMEM((tokens, depth), BF16),
                pltpu.VMEM((tokens, 2 * rb), F32), pltpu.VMEM((tokens, 2 * rb), F32), pltpu.VMEM((tokens, 2 * rb), BF16), pltpu.VMEM((tokens, 2 * rb), BF16),
                pltpu.VMEM((head, tokens), BF16), pltpu.VMEM((head, tokens), BF16), pltpu.VMEM((tokens, head), F32), pltpu.VMEM((tokens, head), F32),
                pltpu.VMEM((head, depth), F32), pltpu.VMEM((head, depth), BF16), pltpu.VMEM((2 * rb, head), BF16), pltpu.VMEM((2 * rb, head), BF16), pltpu.VMEM((8, 2 * rb), F32),
                dma((5,)), dma((2, 6)), dma((2, 4)), dma((3,)), *ring_sems(),
            ],
            compiler_params=pltpu.CompilerParams(collective_id=0, has_side_effects=True, vmem_limit_bytes=VMEM_BYTES),
        )(*stats, *gains, h_mid, d_out, x_in, w_gate, w_up, w_down, w_qkv, w_out.reshape(head, depth))

        late = [(tokens, depth), (depth, width), (depth, ff), (depth, ff), (ff, depth)]
        results = pl.pallas_call(
            functools.partial(second_kernel, size),
            out_shape=tuple(pltpu.VMEM(dims, BF16) for dims in late),
            in_specs=[vmem_spec] * 6 + [any_spec] * 8,
            out_specs=[vmem_spec] * 5,
            scratch_shapes=[
                pltpu.VMEM((tokens, 4), F32), pltpu.VMEM((2, depth), F32),
                pltpu.VMEM((depth, width), BF16), pltpu.VMEM((tokens, width), BF16), pltpu.VMEM((rb, depth), F32), pltpu.VMEM((rb, depth), BF16),
                pltpu.VMEM((tokens, 2 * ff), BF16), pltpu.VMEM((tokens, ff), BF16), pltpu.VMEM((ff, tokens), BF16),
                pltpu.VMEM((2, tokens, blk), BF16), pltpu.VMEM((2, tokens, blk), BF16), pltpu.VMEM((2, tokens, blk), BF16), pltpu.VMEM((blk, tokens), BF16),
                *ring_scratch(rb, depth),
                dma((6,)), dma((2,)), dma((2,)), dma((2,)), *ring_sems(),
            ],
            compiler_params=pltpu.CompilerParams(collective_id=1, has_side_effects=True, vmem_limit_bytes=SECOND_BYTES),
        )(*stats, *gains, h_mid, d_out, x_in, w_qkv, hidden, d_gu, d_qkv, d_mid)

        d_x, d_w_qkv, d_w_gate, d_w_up, d_w_down, d_w_out = pl.pallas_call(
            copy_kernel,
            out_shape=tuple(shape(dims, BF16) for dims in late) + (shape((head, depth), BF16),),
            in_specs=[vmem_spec] * 5 + [any_spec],
            out_specs=[any_spec] * 6,
            scratch_shapes=[pltpu.VMEM((head, depth), BF16), dma((7,))],
            compiler_params=pltpu.CompilerParams(vmem_limit_bytes=COPY_BYTES),
        )(*results, d_w_out)
        return d_x, d_w_qkv, d_w_out.reshape(w_out.shape), d_w_gate, d_w_up, d_w_down

    row_spec = P('dp', None)
    stat_spec = P('dp')
    col_spec = P(None, 'tp')
    in_specs = (row_spec, row_spec, stat_spec, stat_spec, stat_spec, stat_spec, P(None), P(None), col_spec, P('tp', None, None), col_spec, col_spec, P('tp', None), row_spec)
    out_specs = (row_spec, P('dp', 'tp'), P(('dp', 'tp'), None, None), P('dp', 'tp'), P('dp', 'tp'), P(('dp', 'tp'), None))
    return jax.shard_map(device_step, mesh=mesh, in_specs=in_specs, out_specs=out_specs, check_vma=False)
```
